32 devices in a mesh: vocab: 4 (over x, core), expert: 8 (over z, y).
Axes of the slice: x: 2, y: 2, z: 4, core: 2. Of those that a mesh axis runs over, the one named last changes fastest.
Arguments:
- leading_batch_features: bfloat16 [256, 2880], P(('vocab', 'expert')), may hold values from -48 to 48
- sampling_heat_selector: int32 [256], replicated, may hold values from 0 to 3
- output_embedding_matrix: bfloat16 [50272, 2880], P(('vocab', 'expert')), may hold values from -3.354102 to 3.354102
- trailing_batch_features: bfloat16 [512, 2880], P('expert'), may hold values from -6 to 6
- routed_specialist_choice: int32 [512, 4], P('expert'), may hold values from 0 to 31, all different within a row; in each aligned block of 64 rows (0 to 63, 64 to 127, ...) at most 16 rows name the same one
- dispatcher_projection: bfloat16 [2880, 32], replicated, may hold values from -13.416408 to 13.416408
- specialist_gating_matrix: bfloat16 [32, 2880, 1440], P('expert', None, 'vocab'), may hold values from -0.109375 to 0.109375
- specialist_raising_matrix: bfloat16 [32, 2880, 1440], P('expert', None, 'vocab'), may hold values from -0.109375 to 0.109375
- expert_lowering_matrix: bfloat16 [32, 1440, 2880], P('expert', 'vocab'), may hold values from -0.15625 to 0.15625
Outputs:
- lexicon_log_probability: float32 [256, 50272], P(None, ('vocab', 'expert'))
- moe_out: bfloat16 [512, 2880], P('expert', 'vocab')
The draws below stay inside these ranges and needn't reach their ends.
Inputs may be any that keep to these rules, and one draw needn't show every extreme that they name: `routed_specialist_choice`: in the rows of one index of the expert axis no expert is named more than 16 times, a bound that some block reaches.
All inputs are finite; a program needn't handle non-finite values.
Results may differ from the reference program's by a relative error of at most 0.005.
The reference program's roundings to bfloat16 on the way count: a program that leaves them out, or rounds other values in their place, can miss the bound.
Values may be sent and summed in bfloat16 or wider, within the bound.
No kernel may reach another device: no remote copies, remote signals or barrier semaphores. Data moves between devices by JAX's collectives and lax.ppermute only.
A program may use at most 256 MiB of HBM per device.

```python
import math
import jax
import jax.numpy as jnp
import numpy as np
from jax import lax

EMBED_DIMENSION = 2880
FF = 1440
TOPK = 4
TB_DEV = 64
EXPERTS = 32
VOCAB = 50272
LEAD_BATCH_SIZE = 256
TB = 512
CAP = 16
N_EXPERT = 8


def draw_leading_batch_features(key, part):
    key_base = jax.random.fold_in(jax.random.fold_in(key, 11), 0)
    normal_part = jnp.clip(jax.random.normal(key_base, (LEAD_BATCH_SIZE, EMBED_DIMENSION), jnp.float32), -6.0, 6.0)
    return normal_part.astype(jnp.bfloat16)


def draw_output_embedding_matrix(key, part):
    key_base, key_scale = jax.random.split(jax.random.fold_in(key, 23))
    normal_part = jnp.clip(jax.random.normal(key_base, (VOCAB, EMBED_DIMENSION), jnp.float32), -6.0, 6.0) * EMBED_DIMENSION ** (-0.5)
    frac_rows = (jnp.arange(VOCAB, dtype=jnp.float32) / VOCAB)[:, None]
    row_scale = 2.0 * jnp.exp(frac_rows * jnp.log(3.0) + jax.random.uniform(key_scale, (VOCAB, 1), jnp.float32, -0.7, 0.7))
    return (normal_part * row_scale).astype(jnp.bfloat16)


def draw_dispatcher_projection(key, part):
    key_base = jax.random.fold_in(jax.random.fold_in(key, 37), 0)
    normal_part = jnp.clip(jax.random.normal(key_base, (EMBED_DIMENSION, EXPERTS), jnp.float32), -6.0, 6.0) * 2.0 * EMBED_DIMENSION ** (-0.5)
    return normal_part.astype(jnp.bfloat16)


def place_ends(result, stream_key, low, top_value):
    spot = [jax.random.randint(jax.random.fold_in(stream_key, axis), (), 0, length) for axis, length in enumerate(result.shape)]
    longest = result.shape.index(max(result.shape))
    beside = spot[:longest] + [(spot[longest] + 1) % result.shape[longest]] + spot[longest + 1:]
    return result.at[tuple(spot)].set(low).at[tuple(beside)].set(top_value)


def level_of(stream_key, extent, cuts, low, largest):
    loudness, own = 1.0, jax.random.fold_in(stream_key, 6)
    for axis_at, blocks in cuts:
        draws = jnp.exp(jax.random.uniform(jax.random.fold_in(own, axis_at), (blocks,), jnp.float32, low / len(cuts), largest / len(cuts)))
        loudness = loudness * jnp.repeat(draws, extent[axis_at] // blocks).reshape([-1 if axis == axis_at else 1 for axis in range(len(extent))])
    return loudness


def deal_out(rng, own, number, rows, number_of, top, most, lean):
    sequence = jax.random.permutation(rng, number_of)
    heavy_load, common = shares(number_of, rows * top, most, lean, True), shares(number_of, rows * top, most, lean, False)
    places = jnp.arange(number_of)

    def named(lengths, rotation):
        used = int((lengths > 0).sum())
        fixed = max(1, used // 4)
        shifted = fixed + (places - fixed + rotation * (used - fixed)) % max(1, number_of - fixed)
        return jnp.zeros((number_of,), jnp.int32).at[sequence[jnp.where(places < fixed, places, shifted)]].set(jnp.asarray(lengths, jnp.int32))

    lengths = jnp.where(number % 4 == 0, named(heavy_load, number // 4), named(common, number - number // 4 - 1))
    mixed = jax.random.permutation(jax.random.fold_in(own, 3), number_of)
    source_of, receiver = mixed[0:number_of // 2 * 2:2], mixed[1:number_of // 2 * 2:2]
    slack = jnp.minimum(lengths[source_of] - 1, most - lengths[receiver]) // 2
    slack = jnp.where((source_of == sequence[0]) | (receiver == sequence[0]) | (lengths[receiver] == 0), 0, jnp.maximum(slack, 0))
    shifted = jax.random.randint(jax.random.fold_in(own, 4), (number_of // 2,), 0, 1 << 20) % (slack + 1)
    lengths = lengths.at[source_of].add(-shifted).at[receiver].add(shifted)
    items = jnp.searchsorted(jnp.cumsum(lengths), jnp.arange(rows * top), side="right").astype(jnp.int32)
    listing = items.reshape(top, rows).T
    listing = listing[jax.random.permutation(jax.random.fold_in(own, 1), rows)]
    rotation = jax.random.randint(jax.random.fold_in(own, 2), (rows, 1), 0, top)
    return jnp.take_along_axis(listing, (jnp.arange(top)[None, :] + rotation) % top, axis=1)


def shares(number_of, total, reach, slope, full):
    weights = [(1 << 20) // math.isqrt(grade ** slope) + 1 for grade in range(1, number_of + 1)]
    largest = reach if full else min(reach, max(-(-total // number_of), total * weights[0] // sum(weights)))
    least = 1 if total - largest >= number_of - 1 else 0
    given, surplus = [largest] + [least] * (number_of - 1), total - largest - least * (number_of - 1)
    while surplus > 0:
        candidates = [i for i in range(1, number_of) if given[i] < largest] or [i for i in range(1, number_of) if given[i] < reach]
        whole, left = sum([weights[i] for i in candidates]), surplus
        for i in candidates:
            addition = min(reach - given[i], max(1, left * weights[i] // whole), surplus)
            given[i] = given[i] + addition
            surplus = surplus - addition
    return np.array(given)


def noise(own_key, extent, spread, limit, pieces=(), kind=jnp.bfloat16):
    level = level_of(own_key, extent, pieces, -0.22, 0.18) if pieces else 1.0
    entries = jax.random.normal(own_key, extent, jnp.float32) * spread * level
    return jnp.minimum(jnp.maximum(entries, -limit), limit).astype(kind)


def setup_inputs(seed: int = 0) -> dict:
    streams_of = jax.random.split(jax.random.key(seed), 10)
    leading_batch_features = draw_leading_batch_features(jax.random.fold_in(streams_of[9], 71), 0)
    sampling_heat_selector = place_ends(jax.random.randint(streams_of[1], (LEAD_BATCH_SIZE,), 0, 4), jax.random.fold_in(streams_of[1], 1), 0, 3).astype(jnp.int32)
    output_embedding_matrix = draw_output_embedding_matrix(jax.random.fold_in(streams_of[9], 71), 0)
    trailing_batch_features = noise(streams_of[3], (TB, EMBED_DIMENSION), 1.0, 6.0, ((0, 8),))
    routed_specialist_choice_keys = jax.random.split(jax.random.fold_in(streams_of[4], 1), TB // TB_DEV)
    routed_specialist_choice_turns = jax.random.permutation(jax.random.fold_in(streams_of[4], 3), TB // TB_DEV)
    routed_specialist_choice = jax.vmap(lambda own, number: deal_out(jax.random.fold_in(streams_of[4], 2), own, number, TB_DEV, EXPERTS, TOPK, CAP, 2))(routed_specialist_choice_keys, routed_specialist_choice_turns).reshape((TB, TOPK))
    dispatcher_projection = draw_dispatcher_projection(jax.random.fold_in(streams_of[9], 71), 0)
    specialist_gating_matrix = noise(streams_of[6], (EXPERTS, EMBED_DIMENSION, FF), EMBED_DIMENSION ** -0.5, 0.109375, ((0, 8), (2, 4)))
    specialist_raising_matrix = noise(streams_of[7], (EXPERTS, EMBED_DIMENSION, FF), EMBED_DIMENSION ** -0.5, 0.109375, ((0, 8), (2, 4)))
    expert_lowering_matrix = noise(streams_of[8], (EXPERTS, FF, EMBED_DIMENSION), FF ** -0.5, 0.15625, ((0, 8), (1, 4)))
    return dict(leading_batch_features=leading_batch_features, sampling_heat_selector=sampling_heat_selector, output_embedding_matrix=output_embedding_matrix, trailing_batch_features=trailing_batch_features, routed_specialist_choice=routed_specialist_choice, dispatcher_projection=dispatcher_projection, specialist_gating_matrix=specialist_gating_matrix, specialist_raising_matrix=specialist_raising_matrix, expert_lowering_matrix=expert_lowering_matrix)


def slot_numbers(flat_ids, expert_count):
    one_hot = (flat_ids[:, None] == jnp.arange(expert_count, dtype=jnp.int32)[None, :]).astype(jnp.int32)
    earlier = jnp.cumsum(one_hot, axis=0) - one_hot
    return jnp.sum(earlier * one_hot, axis=1).astype(jnp.int32)


def reference(leading_batch_features, sampling_heat_selector, output_embedding_matrix, trailing_batch_features, routed_specialist_choice, dispatcher_projection, specialist_gating_matrix, specialist_raising_matrix, expert_lowering_matrix):
    lexicon_piece_number = math.gcd(LEAD_BATCH_SIZE, 64)
    position_heat_factor = 0.5 + 0.25 * sampling_heat_selector.astype(jnp.float32)

    def lexicon_score_piece(operands):
        token_rows, row_temps = operands
        plain_lexicon_scores = lax.dot_general(token_rows, output_embedding_matrix, (((1,), (1,)), ((), ())), preferred_element_type=jnp.float32)
        heat_divided_scores = plain_lexicon_scores / row_temps[:, None]
        row_max = jnp.max(heat_divided_scores, axis=1)
        row_total = jnp.sum(jnp.exp(heat_divided_scores - row_max[:, None]), axis=1)
        return heat_divided_scores - row_max[:, None] - jnp.log(row_total)[:, None]

    lexicon_log_probability = lax.map(lexicon_score_piece, (leading_batch_features.reshape(LEAD_BATCH_SIZE // lexicon_piece_number, lexicon_piece_number, EMBED_DIMENSION), position_heat_factor.reshape(LEAD_BATCH_SIZE // lexicon_piece_number, lexicon_piece_number)))
    lexicon_log_probability = lexicon_log_probability.reshape(LEAD_BATCH_SIZE, VOCAB)

    router_full = jnp.dot(trailing_batch_features, dispatcher_projection, preferred_element_type=jnp.float32)
    scores = jnp.take_along_axis(router_full, routed_specialist_choice, axis=1)
    gate_probs = jax.nn.softmax(scores, axis=1)
    slots = jax.vmap(lambda ids_block: slot_numbers(ids_block, EXPERTS))(routed_specialist_choice.reshape(N_EXPERT, TB_DEV * TOPK))
    slots = slots.reshape(TB, TOPK)
    block_index = (jnp.arange(TB, dtype=jnp.int32) // TB_DEV).astype(jnp.int32)
    slot_index = (routed_specialist_choice * (N_EXPERT * CAP) + block_index[:, None] * CAP + slots).reshape(-1).astype(jnp.int32)
    token_rows = jnp.repeat(trailing_batch_features, TOPK, axis=0)
    buffer = jnp.zeros((EXPERTS * N_EXPERT * CAP, EMBED_DIMENSION), jnp.bfloat16).at[slot_index].set(token_rows)
    buffer = buffer.reshape(EXPERTS, N_EXPERT * CAP, EMBED_DIMENSION)

    def one_expert(operands):
        expert_rows, w_gate, w_up, w_down = operands
        gate_proj = jnp.dot(expert_rows, w_gate, preferred_element_type=jnp.float32)
        up_proj = jnp.dot(expert_rows, w_up, preferred_element_type=jnp.float32)
        activated = (gate_proj * jax.nn.sigmoid(1.702 * gate_proj) * (up_proj + 1.0)).astype(jnp.bfloat16)
        return jnp.dot(activated, w_down, preferred_element_type=jnp.float32).astype(jnp.bfloat16)

    expert_outs = lax.map(one_expert, (buffer, specialist_gating_matrix, specialist_raising_matrix, expert_lowering_matrix))
    expert_outs = expert_outs.reshape(EXPERTS * N_EXPERT * CAP, EMBED_DIMENSION)
    picked = expert_outs[slot_index].reshape(TB, TOPK, EMBED_DIMENSION).astype(jnp.float32)
    moe_out = jnp.sum(gate_probs[:, :, None] * picked, axis=1).astype(jnp.bfloat16)
    return lexicon_log_probability, moe_out
```

```python
import jax
import jax.numpy as jnp
from jax import lax
from jax.sharding import PartitionSpec as P


LANES = 128
BF16 = jnp.bfloat16
F32 = jnp.float32


def shifted(value, axis, size, step):
    return lax.ppermute(value, axis, [(i, (i + step) % size) for i in range(size)])


def toggled(value, axis, size, bit):
    return lax.ppermute(value, axis, [(i, i ^ bit) for i in range(size)])


def chip_shifted(value, size, step):
    return lax.ppermute(value, "vocab", [(i, (i + 2 * step) % size) for i in range(size)])


def merged(stats, axis, size):
    bit = 1
    while bit < size:
        other = toggled(stats, axis, size, bit)
        top = jnp.maximum(stats[0], other[0])
        total = stats[1] * jnp.exp(stats[0] - top) + other[1] * jnp.exp(other[0] - top)
        stats = jnp.stack([top, total])
        bit *= 2
    return stats


def in_core_order(own, other, core, axis):
    first = jnp.where(core == 0, own, other)
    second = jnp.where(core == 0, other, own)
    return jnp.stack([first, second], axis=axis)


def per_device(lead, heat, embedding, tokens, choice, router, w_gate, w_up, w_down):
    vocab_n, expert_n = lax.axis_size("vocab"), lax.axis_size("expert")
    chips = vocab_n // 2
    v, ex = lax.axis_index("vocab"), lax.axis_index("expert")
    core, chip = v % 2, v // 2
    tok, width = tokens.shape
    top = choice.shape[1]
    local = w_gate.shape[0]
    experts = router.shape[1]
    cap = max(2, 2 * top * tok // experts)
    half = tok // 2
    lead_rows = lead.shape[0]

    spare = -width % LANES
    if spare < top:
        spare += LANES
    tagged = jnp.concatenate(
        [tokens, choice.astype(BF16), jnp.zeros((tok, spare - top), BF16)], axis=1
    )
    part = lax.dynamic_slice_in_dim(tagged, core * half, half, 0)
    parts = [part] + [shifted(part, "expert", expert_n, d) for d in range(1, expert_n)]
    own_half = jnp.stack(parts)
    other_half = toggled(own_half, "vocab", vocab_n, 1)
    rows = in_core_order(own_half, other_half, core, 1).reshape(expert_n * tok, width + spare)

    lead_parts = jnp.stack([lead] + [shifted(lead, "expert", expert_n, d) for d in range(1, expert_n)])
    lead_chips = jnp.stack(
        [lead_parts] + [chip_shifted(lead_parts, vocab_n, d) for d in range(1, chips)]
    )
    lead_other = toggled(lead_chips, "vocab", vocab_n, 1)
    both = in_core_order(lead_chips, lead_other, core, 1)
    chip_at = (chip - jnp.arange(chips)) % chips
    ex_at = (ex - jnp.arange(expert_n)) % expert_n
    both = jnp.stack([lax.dynamic_index_in_dim(both, chip_at[a], 0, False) for a in range(chips)])
    both = jnp.stack(
        [lax.dynamic_index_in_dim(both, ex_at[d], 2, False) for d in range(expert_n)], axis=2
    )
    lead_all = both.reshape(vocab_n * expert_n * lead_rows, width)

    ids = rows[:, width : width + top].reshape(expert_n, tok, top).astype(jnp.int32)
    wanted = ex * local + jnp.arange(local, dtype=jnp.int32)
    named = jnp.any(ids[:, :, :, None] == wanted, axis=2)
    earlier = jnp.arange(tok)[:, None] > jnp.arange(tok)[None, :]
    rank = jnp.einsum(
        "ut,dtl->dul", earlier.astype(BF16), named.astype(BF16), preferred_element_type=F32
    ).astype(jnp.int32)
    spot = jnp.where(named, rank, -1).transpose(2, 0, 1)
    pick = (
        (spot[:, None, None, :, :] == jnp.arange(cap)[None, None, :, None, None])
        & (jnp.arange(expert_n)[:, None, None, None] == jnp.arange(expert_n)[None, None, :, None])
    ).astype(BF16)
    pick = pick.reshape(local * expert_n * cap, expert_n * tok)
    received = jnp.dot(pick, rows[:, :width], preferred_element_type=F32).astype(BF16)
    received = received.reshape(local, expert_n * cap, width)

    gate_proj = jnp.einsum("erd,edf->erf", received, w_gate, preferred_element_type=F32)
    up_proj = jnp.einsum("erd,edf->erf", received, w_up, preferred_element_type=F32)
    activated = (gate_proj * jax.nn.sigmoid(1.702 * gate_proj) * (up_proj + 1.0)).astype(BF16)
    partial = jnp.einsum("erf,efd->erd", activated, w_down, preferred_element_type=F32)
    partial = partial.reshape(local * expert_n * cap, width)

    piece = width // vocab_n
    cols = [partial[:, i * piece : (i + 1) * piece] for i in range(vocab_n)]
    keep = jnp.stack([jnp.where(core == 0, cols[2 * a], cols[2 * a + 1]) for a in range(chips)])
    give = jnp.stack([jnp.where(core == 0, cols[2 * a + 1], cols[2 * a]) for a in range(chips)])
    pair = keep + toggled(give, "vocab", vocab_n, 1)
    total = lax.dynamic_index_in_dim(pair, chip, 0, False)
    pair = pair.astype(BF16)
    for d in range(1, chips):
        leaving = lax.dynamic_index_in_dim(pair, (chip + d) % chips, 0, False)
        total = total + chip_shifted(leaving, vocab_n, d).astype(F32)
    shares = total.astype(BF16).reshape(local, expert_n, cap, piece)

    back = [shares[:, 0]] + [
        shifted(shares[:, d], "expert", expert_n, -d) for d in range(1, expert_n)
    ]
    returned = jnp.stack(back).reshape(expert_n * local * cap, piece)

    scores_all = jnp.dot(tokens, router, preferred_element_type=F32)
    one_hot = (choice[:, :, None] == jnp.arange(experts, dtype=jnp.int32)).astype(F32)
    scores = jnp.sum(scores_all[:, None, :] * one_hot, axis=2)
    gates = jax.nn.softmax(scores, axis=1)
    used = jnp.sum(one_hot, axis=1).astype(BF16)
    place = jnp.dot(earlier.astype(BF16), used, preferred_element_type=F32)
    slot = jnp.sum(place[:, None, :] * one_hot, axis=2).astype(jnp.int32)
    ahead = (choice // local - ex) % expert_n
    at = (ahead * local + choice % local) * cap + slot
    picked = returned[at.reshape(-1)].reshape(tok, top, piece).astype(F32)
    moe_out = jnp.sum(gates[:, :, None] * picked, axis=1).astype(BF16)

    temperature = 0.5 + 0.25 * heat.astype(F32)
    logits = lax.dot_general(
        lead_all, embedding, (((1,), (1,)), ((), ())), preferred_element_type=F32
    )
    scaled = logits / temperature[:, None]
    row_max = jnp.max(scaled, axis=1)
    row_total = jnp.sum(jnp.exp(scaled - row_max[:, None]), axis=1)
    stats = merged(merged(jnp.stack([row_max, row_total]), "vocab", vocab_n), "expert", expert_n)
    log_prob = scaled - stats[0][:, None] - jnp.log(stats[1])[:, None]
    return log_prob, moe_out


def solution(mesh):
    placed = (
        P(("vocab", "expert"), None),
        P(),
        P(("vocab", "expert"), None),
        P("expert", None),
        P("expert", None),
        P(),
        P("expert", None, "vocab"),
        P("expert", None, "vocab"),
        P("expert", "vocab", None),
    )
    return jax.shard_map(
        per_device,
        mesh=mesh,
        in_specs=placed,
        out_specs=(P(None, ("vocab", "expert")), P("expert", "vocab")),
        check_vma=False,
    )
```
